256 devices in a mesh: grp: 32 (over x, z_hi, core), mem: 8 (over y, z_lo).
Axes of the slice: x: 4, y: 4, z: 8 (z_hi: 4, z_lo: 2; z = z_hi * 2 + z_lo), core: 2. Of those that a mesh axis runs over, the one named last changes fastest.
Arguments:
- forcing: float32 [16, 512, 128, 128], P(None, 'grp', 'mem'), may hold values from -8 to 8
- aggregate: int32 [128, 32, 32], P('grp', 'mem'), may hold values from 0 to 8191, as said below
- factors: float32 [64, 128, 128], P('mem'), may hold values from -1.5 to 1.5, as said below
Outputs:
- solution: float32 [16, 512, 128, 128], P(None, 'grp', 'mem')
The draws below stay inside these ranges and needn't reach their ends.
Inputs may be any that keep to these rules, and one draw needn't show every extreme that they name: Coarse unknowns are numbered over the fine blocks with the first block index taken modulo half the number of blocks along the first dimension, consecutive numbers lying close together in the other dimensions, so that an aggregate joins blocks of both halves of the grid; a few blocks take the entry of a block beside them. `factors`: each of the 64 blocks is lower triangular with its diagonal between 0.5 and 1.5.
All inputs are finite; a program needn't handle non-finite values.
Results may differ from the reference program's by a relative error of at most 0.00013.
Values sent between devices are 32-bit elements; how exact they have to be, the bound alone decides.
No kernel may reach another device: no remote copies, remote signals or barrier semaphores. Data moves between devices by JAX's collectives and lax.ppermute only.
A program may use at most 128 MiB of HBM per device.

```python
import math
import jax
import jax.numpy as jnp
from jax import lax

RHS = 16
NC = 8192
BS = 128
PRE = 3
POST = 2
NB = 64
NX = 512
NY = 128
NZ = 128


def draw_forcing(key, part):
    noise_key = jax.random.fold_in(jax.random.fold_in(key, 11), 0)
    base_noise = jax.random.normal(noise_key, (RHS, NX, NY, NZ), jnp.float32)
    values = base_noise
    return jnp.clip(values, -8.0, 8.0)


def draw_aggregate(key, part):
    blk_x = NX // 4
    blk_y = NY // 4
    blk_z = NZ // 4
    fold_x = blk_x // 2
    total = fold_x * blk_y * blk_z
    shape = (blk_x, blk_y, blk_z)
    linear = lax.broadcasted_iota(jnp.int32, shape, 0) % fold_x * (blk_y * blk_z) + lax.broadcasted_iota(jnp.int32, shape, 1) * blk_z + lax.broadcasted_iota(jnp.int32, shape, 2)
    if total >= NC:
        base = linear // (total // NC)
    else:
        base = linear * (NC // total)
    x_next = jnp.concatenate([base[1:], base[-1:]], axis=0)
    x_prev = jnp.concatenate([base[:1], base[:-1]], axis=0)
    y_next = jnp.concatenate([base[:, 1:], base[:, -1:]], axis=1)
    y_prev = jnp.concatenate([base[:, :1], base[:, :-1]], axis=1)
    picks = jax.random.randint(jax.random.fold_in(key, 37), shape, 0, 24)
    moved = jnp.where(picks == 0, x_next, jnp.where(picks == 1, x_prev, jnp.where(picks == 2, y_next, jnp.where(picks == 3, y_prev, base))))
    return moved.astype(jnp.int32)


def draw_factors(key, part):
    first_key, second_key = jax.random.split(jax.random.fold_in(key, 23))
    lower = jnp.clip(jax.random.normal(first_key, (NB, BS, BS), jnp.float32) * (0.5 / math.sqrt(BS)), -1.5, 1.5)
    diag_vals = jax.random.uniform(second_key, (NB, BS), jnp.float32, 0.5, 1.5)
    row_ids = lax.broadcasted_iota(jnp.int32, (BS, BS), 0)
    col_ids = lax.broadcasted_iota(jnp.int32, (BS, BS), 1)
    strict = jnp.where(row_ids > col_ids, lower, 0.0)
    return strict + jnp.where(row_ids == col_ids, diag_vals[:, :, None], 0.0)


def setup_inputs(seed: int = 0) -> dict:
    streams_of = jax.random.split(jax.random.key(seed), 4)
    forcing = draw_forcing(jax.random.fold_in(streams_of[3], 71), 0)
    aggregate = draw_aggregate(jax.random.fold_in(streams_of[3], 71), 0)
    factors = draw_factors(jax.random.fold_in(streams_of[3], 71), 0)
    return {"forcing": forcing, "aggregate": aggregate, "factors": factors}


relaxation = 0.8


def apply_operator(values):
    padded = jnp.pad(values, 1)
    beside = padded[2:, 1:-1, 1:-1] + padded[:-2, 1:-1, 1:-1]
    beside = beside + padded[1:-1, 2:, 1:-1] + padded[1:-1, :-2, 1:-1]
    beside = beside + padded[1:-1, 1:-1, 2:] + padded[1:-1, 1:-1, :-2]
    return 6.0 * values - beside


def restrict_blocks(residual, aggregate):
    blk_x, blk_y, blk_z = aggregate.shape
    means = residual.reshape(blk_x, 4, blk_y, 4, blk_z, 4).mean(axis=(1, 3, 5))
    return jax.ops.segment_sum(means.reshape(-1), aggregate.reshape(-1), num_segments=NC)


def prolong_blocks(coarse_fix, aggregate):
    blk_x, blk_y, blk_z = aggregate.shape
    picked = jnp.take(coarse_fix, aggregate.reshape(-1)).reshape(blk_x, 1, blk_y, 1, blk_z, 1)
    return jnp.broadcast_to(picked, (blk_x, 4, blk_y, 4, blk_z, 4)).reshape(blk_x * 4, blk_y * 4, blk_z * 4)


def reference(forcing, aggregate, factors):
    weight = relaxation / 6.0

    def one_side(source):
        smoothed = weight * source
        for repeat in range(PRE - 1):
            smoothed = smoothed + weight * (source - apply_operator(smoothed))
        residual = source - apply_operator(smoothed)
        coarse_rhs = restrict_blocks(residual, aggregate).reshape(NB, BS)
        inner = jnp.einsum('bij,bj->bi', factors, coarse_rhs, precision=lax.Precision.HIGHEST)
        coarse_fix = jnp.einsum('bij,bi->bj', factors, inner, precision=lax.Precision.HIGHEST).reshape(NC)
        lifted = prolong_blocks(coarse_fix, aggregate)
        solution = smoothed + (lifted - weight * apply_operator(lifted))
        for repeat in range(POST):
            solution = solution + weight * (source - apply_operator(solution))
        return solution

    return lax.map(one_side, forcing)
```

```python
import functools
import math

import jax
import jax.numpy as jnp
import numpy as np
from jax import lax
from jax.experimental import pallas as pl
from jax.experimental.pallas import tpu as pltpu
from jax.sharding import PartitionSpec as P

NC = 8192
RHS = 16
BS = 128
SIDE = 16
NZ = 128
RIM = 4
WIDE = SIDE + 2 * RIM
BLK = WIDE // 4
NBLK = BLK * BLK
WEIGHT = 0.8 / 6.0
BOTH = ("grp", "mem")
F32, BF16 = jnp.float32, jnp.bfloat16


def line_operator(size):
    return (
        (1.0 / 3.0 - 2.0 * WEIGHT) * np.eye(size)
        + WEIGHT * np.eye(size, k=1)
        + WEIGHT * np.eye(size, k=-1)
    )


def block_sums(size):
    return np.kron(np.eye(size // 4), np.ones((1, 4)))


def side_tables():
    out = np.zeros((3, 4, BLK, SIDE))
    for place in range(3):
        keep = np.ones(WIDE)
        if place == 1:
            keep[:RIM] = 0
        if place == 2:
            keep[-RIM:] = 0
        step = line_operator(WIDE) * keep[:, None] * keep[None, :]
        power = np.diag(keep)
        for p in range(4):
            out[place, p] = (block_sums(WIDE) @ power)[:, RIM:-RIM]
            power = power @ step
    return out


def split_const(value):
    value = np.asarray(value, np.float32)
    high = value.astype(jnp.bfloat16)
    low = (value - high.astype(np.float32)).astype(jnp.bfloat16)
    return np.stack([high, low])


@functools.cache
def tables():
    side = side_tables()
    plane = np.zeros((3, 3, 4, NBLK, SIDE * SIDE))
    for j in range(4):
        for p in range(4 - j):
            q = 3 - j - p
            factor = 6.0 / (math.factorial(p) * math.factorial(q) * math.factorial(j)) / 64.0
            plane[:, :, j] += factor * np.einsum("aXx,bYy->abXYxy", side[:, p], side[:, q]).reshape(
                3, 3, NBLK, SIDE * SIDE
            )
    plane = split_const(plane.reshape(9, 4 * NBLK, SIDE * SIDE)).transpose(1, 0, 2, 3)
    power = np.eye(NZ)
    lines = []
    for j in range(4):
        lines.append(power @ block_sums(NZ).T)
        power = power @ line_operator(NZ)
    lines = np.stack(lines)
    gather_z = np.tile(lines.reshape(4 * NZ, NZ // 4), (1, 4))
    spread_z = 64.0 * np.tile(lines.transpose(2, 0, 1).reshape(NZ // 4, 4 * NZ), (4, 1))
    return plane, split_const(gather_z), split_const(spread_z)


def split(value):
    high = value.astype(BF16)
    return high, (value - high.astype(F32)).astype(BF16)


def dot(a, b, dims=(((1,), (0,)), ((), ()))):
    return lax.dot_general(a, b, dims, preferred_element_type=F32)


def dot3(a, b, dims=(((1,), (0,)), ((), ()))):
    return dot(a[0], b[0], dims) + dot(a[0], b[1], dims) + dot(a[1], b[0], dims)


GROUPS = NBLK // 4


def slot_lanes(rows):
    return lax.broadcasted_iota(jnp.int32, (rows, NZ), 1) // (NZ // 4)


def restrict_kernel(place_ref, f_ref, plane_ref, line_ref, out_ref, part_ref):
    plane = (plane_ref[0, 0], plane_ref[0, 1])
    for k in range(0, RHS, 2):
        pair = [f_ref[k + i].reshape(SIDE * SIDE, NZ) for i in range(2)]
        value = dot3(plane, split(jnp.concatenate(pair, axis=1)))
        for i in range(2):
            part_ref[pl.ds(k + i, 4 * NBLK, stride=RHS), :] = value[:, i * NZ : (i + 1) * NZ]
    line = (line_ref[0], line_ref[1])
    slots = slot_lanes(GROUPS * RHS)
    total = jnp.zeros((GROUPS * RHS, NZ), F32)
    for s in range(4):
        columns = []
        for j in range(4):
            rows = [
                part_ref[pl.ds((j * NBLK + g * 4 + s) * RHS, RHS), :] for g in range(GROUPS)
            ]
            columns.append(jnp.concatenate(rows, axis=0))
        value = dot3(split(jnp.concatenate(columns, axis=1)), line)
        total = jnp.where(slots == s, value, total)
    out_ref[...] = total


def full(shape):
    return pl.BlockSpec(shape, lambda i, place: (0,) * len(shape))


def restrict_own(forcing, place):
    plane, gather_z, _ = tables()
    return pl.pallas_call(
        restrict_kernel,
        out_shape=jax.ShapeDtypeStruct((GROUPS * RHS, NZ), F32),
        grid_spec=pltpu.PrefetchScalarGridSpec(
            num_scalar_prefetch=1,
            grid=(1,),
            in_specs=[
                full(forcing.shape),
                pl.BlockSpec((1,) + plane.shape[1:], lambda i, place: (place[0], 0, 0, 0)),
                full(gather_z.shape),
            ],
            out_specs=full((GROUPS * RHS, NZ)),
            scratch_shapes=[pltpu.VMEM((4 * NBLK * RHS, NZ), F32)],
        ),
        cost_estimate=pl.CostEstimate(
            flops=6 * 10**9, bytes_accessed=3 * 2**20, transcendentals=0
        ),
        name="restrict",
    )(place, forcing, jnp.asarray(plane), jnp.asarray(gather_z))


def correct_kernel(place_ref, c_ref, q_ref, plane_ref, line_ref, out_ref, part_ref):
    value = c_ref[...]
    line = (line_ref[0], line_ref[1])
    slots = slot_lanes(GROUPS * RHS)
    for s in range(4):
        spread = dot3(split(jnp.where(slots == s, value, 0.0)), line)
        for j in range(4):
            for g in range(GROUPS):
                part_ref[pl.ds((j * NBLK + g * 4 + s) * RHS, RHS), :] = spread[
                    g * RHS : (g + 1) * RHS, j * NZ : (j + 1) * NZ
                ]
    plane = (plane_ref[0, 0], plane_ref[0, 1])
    for k in range(0, RHS, 2):
        pair = [part_ref[pl.ds(k + i, 4 * NBLK, stride=RHS), :] for i in range(2)]
        value = dot3(plane, split(jnp.concatenate(pair, axis=1)), (((0,), (0,)), ((), ())))
        for i in range(2):
            own = value[:, i * NZ : (i + 1) * NZ].reshape(SIDE, SIDE, NZ)
            out_ref[k + i] = q_ref[k + i] + own


def add_correction(smooth, coarse, place):
    plane, _, spread_z = tables()
    return pl.pallas_call(
        correct_kernel,
        out_shape=jax.ShapeDtypeStruct(smooth.shape, F32),
        grid_spec=pltpu.PrefetchScalarGridSpec(
            num_scalar_prefetch=1,
            grid=(1,),
            in_specs=[
                full(coarse.shape),
                full(smooth.shape),
                pl.BlockSpec((1,) + plane.shape[1:], lambda i, place: (place[0], 0, 0, 0)),
                full(spread_z.shape),
            ],
            out_specs=full(smooth.shape),
            scratch_shapes=[pltpu.VMEM((4 * NBLK * RHS, NZ), F32)],
        ),
        cost_estimate=pl.CostEstimate(
            flops=6 * 10**9, bytes_accessed=5 * 2**20, transcendentals=0
        ),
        name="correct",
    )(place, coarse, smooth, jnp.asarray(plane), jnp.asarray(spread_z))


SWEEPS = 4


def smooth_kernel(inside_ref, f_ref, ylo_ref, yhi_ref, xlo_ref, xhi_ref, out_ref, src, one, two):
    low_x, high_x = inside_ref[0], inside_ref[1]
    row = lax.broadcasted_iota(jnp.int32, (WIDE, NZ), 0)
    low_y = jnp.where(row < RIM, inside_ref[2].astype(F32), 1.0)
    in_y = jnp.where(row >= RIM + SIDE, inside_ref[3].astype(F32), low_y)
    lane = lax.broadcasted_iota(jnp.int32, (WIDE, NZ), 1)
    has_lower, has_upper = lane > 0, lane < NZ - 1

    def load(k):
        for x in range(RIM):
            src[x] = xlo_ref[k, x]
            src[RIM + SIDE + x] = xhi_ref[k, x]
        for x in range(SIDE):
            src[RIM + x, pl.ds(0, RIM), :] = ylo_ref[k, x]
            src[RIM + x, pl.ds(RIM, SIDE), :] = f_ref[k, x]
            src[RIM + x, pl.ds(RIM + SIDE, RIM), :] = yhi_ref[k, x]
        for x in range(WIDE):
            value = WEIGHT * src[x]
            src[x] = value
            one[x] = value

    def sweep(t, old, new, k):
        for x in range(t, WIDE - t):
            here = old[x]
            near = old[x - 1] + old[x + 1]
            near += pltpu.roll(here, 1, 0) + pltpu.roll(here, WIDE - 1, 0)
            near += jnp.where(has_lower, pltpu.roll(here, 1, 1), 0.0)
            near += jnp.where(has_upper, pltpu.roll(here, NZ - 1, 1), 0.0)
            value = src[x] + (1.0 - 6.0 * WEIGHT) * here + WEIGHT * near
            if t == SWEEPS:
                out_ref[k, x - RIM] = value[RIM : RIM + SIDE]
                continue
            value = value * in_y
            if x < RIM:
                value = value * low_x.astype(F32)
            if x >= RIM + SIDE:
                value = value * high_x.astype(F32)
            new[x] = value

    def body(k, carry):
        load(k)
        bufs = (one, two)
        for t in range(1, SWEEPS + 1):
            sweep(t, bufs[(t - 1) % 2], bufs[t % 2], k)
        return carry

    lax.fori_loop(0, f_ref.shape[0], body, 0)


def smooth_all(forcing, ylo, yhi, xlo, xhi, inside):
    steps = 4
    each = RHS // steps

    def part(value):
        return pl.BlockSpec((each,) + value.shape[1:], lambda i, place: (i, 0, 0, 0))

    args = (forcing, ylo, yhi, xlo, xhi)
    return pl.pallas_call(
        smooth_kernel,
        out_shape=jax.ShapeDtypeStruct(forcing.shape, F32),
        grid_spec=pltpu.PrefetchScalarGridSpec(
            num_scalar_prefetch=1,
            grid=(steps,),
            in_specs=[part(a) for a in args],
            out_specs=part(forcing),
            scratch_shapes=[pltpu.VMEM((WIDE, WIDE, NZ), F32)] * 3,
        ),
        cost_estimate=pl.CostEstimate(
            flops=10**10, bytes_accessed=7 * 2**20, transcendentals=0
        ),
        name="smooth",
    )(inside, *args)


def shift_pairs(size):
    up = [(i, i + 1) for i in range(size - 1)]
    return up, [(b, a) for a, b in up]


def rim_of(value, axis, dim, width):
    size, length = lax.axis_size(axis), value.shape[dim]
    up, down = shift_pairs(size)
    low = lax.ppermute(lax.slice_in_dim(value, length - width, length, axis=dim), axis, up)
    high = lax.ppermute(lax.slice_in_dim(value, 0, width, axis=dim), axis, down)
    return low, high


def with_rim(value, axis, dim, width):
    low, high = rim_of(value, axis, dim, width)
    return jnp.concatenate([low, value, high], axis=dim)


def coarse_everywhere(local, ids, factors):
    members = lax.axis_size("mem")
    slabs = lax.axis_size("grp")
    owned = NC // BS // members
    shares = slabs // owned
    sides = RHS // shares
    summed = jax.ops.segment_sum(local.T, ids, num_segments=NC)
    parts = summed.reshape(members, owned, BS, shares, sides).transpose(1, 3, 0, 4, 2)
    parts = parts.reshape(slabs * members, sides, BS)
    pieces = lax.all_to_all(parts, BOTH, 0, 0, tiled=True)
    mine = jnp.sum(pieces, axis=0)
    factor = lax.dynamic_index_in_dim(factors, lax.axis_index("grp") // shares, 0, keepdims=False)
    inner = jnp.einsum("kj,ij->ki", mine, factor, precision=lax.Precision.HIGHEST)
    fix = jnp.einsum("ki,ij->kj", inner, factor, precision=lax.Precision.HIGHEST)
    copies = jnp.broadcast_to(fix, (slabs * members, *fix.shape))
    fixes = lax.all_to_all(copies, BOTH, 0, 0, tiled=True)
    fixes = fixes.reshape(owned, shares, members, sides, BS).transpose(1, 3, 2, 0, 4)
    return jnp.take(fixes.reshape(RHS, NC), ids, axis=1)


def shards(forcing, aggregate, factors):
    slab, member = lax.axis_index("grp"), lax.axis_index("mem")
    slabs, members = lax.axis_size("grp"), lax.axis_size("mem")

    def place_of(index, size):
        return jnp.where(index == 0, 1, jnp.where(index == size - 1, 2, 0))

    place = (place_of(slab, slabs) * 3 + place_of(member, members)).reshape(1).astype(jnp.int32)
    inside = jnp.stack([slab > 0, slab < slabs - 1, member > 0, member < members - 1])
    inside = inside.astype(jnp.int32)

    ids = with_rim(with_rim(aggregate, "grp", 0, 1), "mem", 1, 1).reshape(-1)
    ylo, yhi = rim_of(forcing, "mem", 2, RIM)
    local = restrict_own(forcing, place)
    local = local.reshape(GROUPS, RHS, NZ).transpose(1, 0, 2).reshape(RHS, GROUPS * NZ)
    picked = coarse_everywhere(local, ids, factors)
    coarse = picked.reshape(RHS, GROUPS, NZ).transpose(1, 0, 2).reshape(GROUPS * RHS, NZ)

    def edge(at):
        return jnp.concatenate(
            [lax.slice_in_dim(v, at, at + RIM, axis=1) for v in (ylo, forcing, yhi)], axis=2
        )

    up, down = shift_pairs(slabs)
    xlo = lax.ppermute(edge(SIDE - RIM), "grp", up)
    xhi = lax.ppermute(edge(0), "grp", down)
    smooth = smooth_all(forcing, ylo, yhi, xlo, xhi, inside)
    return add_correction(smooth, coarse, place)


def solution(mesh):
    placed = (P(None, "grp", "mem", None), P("grp", "mem", None), P("mem", None, None))
    return jax.shard_map(
        shards, mesh=mesh, in_specs=placed, out_specs=P(None, "grp", "mem", None), check_vma=False
    )
```
